32 devices in a mesh: rep: 8 (over y, x, core), shard: 4 (over z).
Axes of the slice: x: 2, y: 2, z: 4, core: 2. Of those that a mesh axis runs over, the one named last changes fastest.
Arguments:
- deltas: bfloat16 [8, 512, 4096], P('rep', 'shard'), may hold values from -6 to 6
- presence: int32 [8], replicated, may hold values from 0 to 1, as said below
- owner_of: int32 [8], replicated, may hold values from 0 to 7, each once
- outer_params: float32 [512, 4096], P('shard', 'rep'), may hold values from -6 to 6
- momentum: float32 [512, 4096], P('shard', 'rep'), may hold values from -4 to 4
Outputs:
- new_weights: bfloat16 [512, 4096], P('shard')
- new_outer: float32 [512, 4096], P('shard', 'rep')
- new_momentum: float32 [512, 4096], P('shard', 'rep')
The draws below stay inside these ranges and needn't reach their ends.
Inputs may be any that keep to these rules, and one draw needn't show every extreme that they name: `presence`: at least one replica group is present.
All inputs are finite; a program needn't handle non-finite values.
Results may differ from the reference program's by a relative error of at most 0.0075.
Values may be sent and summed in bfloat16 or wider, within the bound.
No kernel may reach another device: no remote copies, remote signals or barrier semaphores. Data moves between devices by JAX's collectives and lax.ppermute only.
A program may use at most 64 MiB of HBM per device.

```python
import jax
import jax.numpy as jnp
from jax import lax

D = 4096
ROWS = 512
REPS = 8
BLOCK = 512


def draw_presence(key, part):
    first = jax.random.fold_in(key, 11)
    second = jax.random.fold_in(key, 12)
    flags = jax.random.randint(first, (REPS,), 0, 2).astype(jnp.int32)
    chosen = jax.random.randint(second, (), 0, REPS)
    return flags.at[chosen].set(1).astype(jnp.int32)


def raised(drawn, own_key, source, target, shards_of, factor):
    owner, partner = [(jnp.arange(drawn.shape[dim]) // (drawn.shape[dim] // shards_of)).reshape([-1 if axis == dim else 1 for axis in range(drawn.ndim)]) for dim in (source, target)]
    chosen = jax.random.permutation(own_key, shards_of)[partner]
    strong = (owner == chosen) | (owner == (partner + shards_of // 2) % shards_of)
    return jnp.where(strong, factor * drawn, drawn)


def shard_levels(rng, shape, split, smallest, top_value):
    def one(axis_at, parts):
        draws = jax.random.uniform(jax.random.fold_in(jax.random.fold_in(rng, 6), axis_at), (parts,), jnp.float32, smallest / len(split), top_value / len(split))
        return jnp.repeat(jnp.exp(draws), shape[axis_at] // parts).reshape((-1,) + (1,) * (len(shape) - axis_at - 1))

    factor_of = one(*split[0])
    for cut in split[1:]:
        factor_of = factor_of * one(*cut)
    return factor_of


def gaussian(rng, extent, scale, bound, cuts=(), held_as=jnp.bfloat16):
    drawn = jax.random.normal(rng, extent, jnp.float32) * scale
    if len(cuts) > 0:
        drawn = shard_levels(rng, extent, cuts, -0.22, 0.18) * drawn
    return jnp.clip(drawn, min=-bound, max=bound).astype(held_as)


def bell_draw_with(own_key, extent, spread, bound, pieces, heavy, dtype=jnp.bfloat16):
    values = spread * jax.random.normal(own_key, extent, jnp.float32)
    if pieces:
        values = values * shard_levels(own_key, extent, pieces, -0.22, 0.18)
    return jnp.clip(raised(values, jax.random.fold_in(own_key, 3), *heavy), -bound, bound).astype(dtype)


def setup_inputs(seed: int = 0) -> dict:
    key_list = jax.random.split(jax.random.key(seed), 6)
    deltas = bell_draw_with(key_list[0], (REPS, ROWS, D), 1.0, 6.0, ((0, 8), (1, 4)), (0, 2, 8, 2.0))
    presence = draw_presence(jax.random.fold_in(key_list[5], 71), 0)
    owner_of = jax.random.permutation(key_list[2], REPS).astype(jnp.int32)
    outer_params = gaussian(key_list[3], (ROWS, D), 1.0, 6.0, ((0, 4), (1, 8)), jnp.float32)
    momentum = gaussian(key_list[4], (ROWS, D), 0.5, 4.0, ((0, 4), (1, 8)), jnp.float32)
    return {"deltas": deltas, "presence": presence, "owner_of": owner_of, "outer_params": outer_params, "momentum": momentum}


def reference(deltas, presence, owner_of, outer_params, momentum):
    present = presence.astype(jnp.float32)
    count = jnp.sum(present)

    def add_group(total, item):
        flag, delta = item
        return total + flag * delta.astype(jnp.float32), None

    start = jnp.zeros((ROWS, D), jnp.float32)
    total, unused = lax.scan(add_group, start, (present, deltas))
    average = total / count
    blocks = average.reshape(ROWS, REPS, BLOCK)
    slotted = jnp.take(blocks, owner_of.astype(jnp.int32), axis=1).reshape(ROWS, D)
    new_momentum = 0.9 * momentum + slotted
    new_outer = outer_params - 0.7 * (slotted + 0.9 * new_momentum)
    inverse = jnp.argsort(owner_of).astype(jnp.int32)
    natural = jnp.take(new_outer.reshape(ROWS, REPS, BLOCK), inverse, axis=1).reshape(ROWS, D)
    new_weights = natural.astype(jnp.bfloat16)
    return (new_weights, new_outer, new_momentum)
```

```python
import jax
import jax.numpy as jnp
from jax import lax
from jax.sharding import PartitionSpec as P


def shards(deltas, presence, owner_of, outer_params, momentum):
    groups = lax.axis_size("rep")
    pair = 2 if groups % 2 == 0 else 1
    chips = groups // pair
    flips = chips & (chips - 1) == 0
    rows = deltas.shape[1]
    width = deltas.shape[2] // groups
    me = lax.axis_index("rep")
    chip, core = me // pair, me % pair

    def target(at, step):
        return at ^ step if flips else (at + step) % chips

    def origin(at, step):
        return at ^ step if flips else (at - step) % chips

    def across(x, step):
        return lax.ppermute(x, "rep", [(i, target(i // pair, step) * pair + i % pair) for i in range(groups)])

    def partner(x):
        return lax.ppermute(x, "rep", [(i, i ^ 1) for i in range(groups)])

    def block(index):
        return lax.dynamic_slice(deltas[0], (0, owner_of[index] * width), (rows, width))

    present = presence.astype(jnp.float32)
    count = jnp.sum(present)
    own_flag = present[me]
    sums = [block(target(chip, s) * pair + core).astype(jnp.float32) * own_flag for s in range(chips)]
    if pair == 2:
        sent = jnp.stack([block(target(chip, s) * pair + 1 - core) for s in range(chips)])
        other = partner(sent)
        other_flag = present[me ^ 1]
        sums = [a + other[s].astype(jnp.float32) * other_flag for s, a in enumerate(sums)]
    total = sums[0]
    for s in range(1, chips):
        total = total + across(sums[s].astype(jnp.bfloat16), s).astype(jnp.float32)
    average = total / count
    new_momentum = 0.9 * momentum + average
    new_outer = outer_params - 0.7 * (average + 0.9 * new_momentum)
    shipped = new_outer.astype(jnp.bfloat16)
    got = jnp.stack([shipped] + [across(shipped, s) for s in range(1, chips)])
    parts = [(core, got)]
    if pair == 2:
        parts.append((1 - core, partner(got)))
    new_weights = jnp.zeros((rows, groups * width), jnp.bfloat16)
    for from_core, held in parts:
        for s in range(chips):
            at = owner_of[origin(chip, s) * pair + from_core] * width
            new_weights = lax.dynamic_update_slice(new_weights, held[s], (0, at))
    return (new_weights, new_outer, new_momentum)


def solution(mesh):
    return jax.shard_map(
        shards,
        mesh=mesh,
        in_specs=(P("rep", "shard", None), P(), P(), P("shard", "rep"), P("shard", "rep")),
        out_specs=(P("shard", None), P("shard", "rep"), P("shard", "rep")),
        check_vma=False,
    )
```

```python
import jax
import jax.numpy as jnp
from jax import lax
from jax.experimental import pallas as pl
from jax.experimental.pallas import tpu as pltpu
from jax.sharding import PartitionSpec as P

SMEM = pl.BlockSpec(memory_space=pltpu.SMEM)
VMEM = pl.BlockSpec(memory_space=pltpu.VMEM)
ANY = pl.BlockSpec(memory_space=pl.ANY)


def vmem(x):
    return pltpu.with_memory_space_constraint(x, pltpu.VMEM)


def shards(deltas, presence, owner_of, outer_params, momentum):
    groups = lax.axis_size("rep")
    pair = 2 if groups % 2 == 0 else 1
    chips = groups // pair
    flips = chips & (chips - 1) == 0
    rows = deltas.shape[1]
    width = deltas.shape[2] // groups
    bf16, f32 = jnp.bfloat16, jnp.float32

    def target(at, step):
        return at ^ step if flips else (at + step) % chips

    def origin(at, step):
        return at ^ step if flips else (at - step) % chips

    def across(x, step):
        return lax.ppermute(x, "rep", [(i, target(i // pair, step) * pair + i % pair) for i in range(groups)])

    def partner(x):
        return lax.ppermute(x, "rep", [(i, i ^ 1) for i in range(groups)])

    def where():
        me = lax.axis_index("rep")
        return me // pair, me % pair

    def columns(owner, ref, at):
        return ref.at[:, pl.ds(pl.multiple_of(owner[at] * width, width), width)]

    def load(owner, delta, *refs):
        outs, sem = refs[:-1], refs[-1]
        chip, core = where()
        copies = []
        for side, out in enumerate(outs):
            for s in range(chips):
                at = target(chip, s) * pair + (core + side) % pair
                copies.append(pltpu.make_async_copy(columns(owner, delta.at[0], at), out.at[s], sem.at[side, s]))
        for copy in reversed(copies):
            copy.start()
        for copy in copies:
            copy.wait()

    blocks = jax.ShapeDtypeStruct((chips, rows, width), bf16)
    held = pl.pallas_call(
        load,
        in_specs=[SMEM, ANY],
        out_specs=[VMEM] * pair,
        out_shape=[pltpu.VMEM((chips, rows, width), bf16)] * pair,
        scratch_shapes=[pltpu.SemaphoreType.DMA((pair, chips))],
        name="load",
    )(owner_of, deltas)
    arrived = [held[0]] + [partner(x) for x in held[1:]]

    def pair_sum(flag, *refs):
        ins, outs = refs[:pair], refs[pair:]
        me = lax.axis_index("rep")
        flags = [flag[me].astype(f32), flag[me ^ 1].astype(f32)][:pair]
        for s in range(chips):
            value = sum(x[s].astype(f32) * p for x, p in zip(ins, flags))
            outs[s][...] = value.astype(outs[s].dtype)

    sums = pl.pallas_call(
        pair_sum,
        in_specs=[SMEM] + [VMEM] * pair,
        out_specs=[VMEM] * chips,
        out_shape=[pltpu.VMEM((rows, width), bf16 if s else f32) for s in range(chips)],
        name="pair_sum",
    )(presence, *[vmem(x) for x in arrived])
    total = sums[0]
    for s in range(1, chips):
        total = total + across(sums[s], s).astype(f32)
    count = jnp.sum(presence.astype(f32))
    average = total / count
    new_momentum = 0.9 * momentum + average
    new_outer = outer_params - 0.7 * (average + 0.9 * new_momentum)
    shipped = new_outer.astype(bf16)
    got = jnp.stack([shipped] + [across(shipped, s) for s in range(1, chips)])
    parts = [got] + [partner(got)] * (pair - 1)

    def place(owner, *refs):
        ins, out, sem = refs[:pair], refs[pair], refs[pair + 1]
        chip, core = where()
        copies = []
        for side, x in enumerate(ins):
            for s in range(chips):
                at = origin(chip, s) * pair + (core + side) % pair
                copies.append(pltpu.make_async_copy(x.at[s], columns(owner, out, at), sem.at[side, s]))
        for copy in copies:
            copy.start()
        for copy in copies:
            copy.wait()

    new_weights = pl.pallas_call(
        place,
        in_specs=[SMEM] + [VMEM] * pair,
        out_specs=ANY,
        out_shape=jax.ShapeDtypeStruct((rows, groups * width), bf16),
        scratch_shapes=[pltpu.SemaphoreType.DMA((pair, chips))],
        name="place",
    )(owner_of, *[vmem(x) for x in parts])
    return (new_weights, new_outer, new_momentum)


def solution(mesh):
    return jax.shard_map(
        shards,
        mesh=mesh,
        in_specs=(P("rep", "shard", None), P(), P(), P("shard", "rep"), P("shard", "rep")),
        out_specs=(P("shard", None), P("shard", "rep"), P("shard", "rep")),
        check_vma=False,
    )
```

```python
import jax
import jax.numpy as jnp
from jax import lax
from jax.experimental import pallas as pl
from jax.experimental.pallas import tpu as pltpu
from jax.sharding import PartitionSpec as P


SMEM = pl.BlockSpec(memory_space=pltpu.SMEM)
VMEM = pl.BlockSpec(memory_space=pltpu.VMEM)
ANY = pl.BlockSpec(memory_space=pl.ANY)
HBM = pl.BlockSpec(memory_space=pltpu.HBM)


def vmem(x):
    return pltpu.with_memory_space_constraint(x, pltpu.VMEM)


def smem(x):
    return pltpu.with_memory_space_constraint(x, pltpu.SMEM)


def shards(deltas, presence, owner_of, outer_params, momentum):
    groups = lax.axis_size("rep")
    chips = groups // 2
    rows = deltas.shape[1]
    width = deltas.shape[2] // groups
    bf16, f32 = jnp.bfloat16, jnp.float32
    flips = sorted(range(chips), key=lambda m: (m.bit_count(), m))

    def direct(x, s):
        return lax.ppermute(x, "rep", [(i, i ^ 2 * flips[s]) for i in range(groups)])

    def swap(x):
        return lax.ppermute(x, "rep", [(i, i ^ 1) for i in range(groups)])

    def where():
        me = lax.axis_index("rep")
        return me // 2, me % 2

    def device(chip, core, s):
        return (chip ^ flips[s]) * 2 + core

    def columns(owner, at):
        return pl.ds(pl.multiple_of(owner[at] * width, width), width)

    def own_flag(flag):
        return flag[lax.axis_index("rep")].astype(f32)

    def tile(*lead, dtype=bf16):
        return pltpu.VMEM((*lead, rows, width), dtype)

    later = [*range(2, chips), 0]

    def load(owner_hbm, flag_hbm, delta, owner, flag, whole, head, tail, sem):
        copies = [
            pltpu.make_async_copy(delta.at[0], whole, sem.at[0]),
            pltpu.make_async_copy(owner_hbm, owner, sem.at[1]),
            pltpu.make_async_copy(flag_hbm, flag, sem.at[2]),
        ]
        for copy in copies:
            copy.start()
        for copy in reversed(copies):
            copy.wait()
        chip, core = where()
        own = own_flag(flag)

        def masked(s):
            return (whole[:, columns(owner, device(chip, 1 - core, s))].astype(f32) * own).astype(bf16)

        head[...] = masked(1)
        for i, s in enumerate(later):
            tail[i] = masked(s)

    owner_of, presence, whole, head, tail = pl.pallas_call(
        load,
        in_specs=[ANY] * 3,
        out_specs=[SMEM] * 2 + [VMEM] * 3,
        out_shape=[pltpu.SMEM((groups,), jnp.int32)] * 2
        + [pltpu.VMEM((rows, groups * width), bf16), tile(), tile(chips - 1)],
        scratch_shapes=[pltpu.SemaphoreType.DMA((3,))],
        name="load",
    )(owner_of, presence, deltas)
    owner_of, presence, whole = smem(owner_of), smem(presence), vmem(whole)
    head = swap(head)
    tail = swap(tail)

    def add(owner, flag, whole, got, s):
        chip, core = where()
        mine = whole[:, columns(owner, device(chip, core, s))].astype(f32)
        return mine * own_flag(flag) + got.astype(f32)

    def sum_head(owner, flag, whole, got, out):
        out[...] = add(owner, flag, whole, got[...], 1).astype(bf16)

    def sum_tail(owner, flag, whole, got, *outs):
        for i, s in enumerate(later):
            outs[i][...] = add(owner, flag, whole, got[i], s).astype(outs[i].dtype)

    head = pl.pallas_call(
        sum_head,
        in_specs=[SMEM] * 2 + [VMEM] * 2,
        out_specs=VMEM,
        out_shape=tile(),
        name="sum_head",
    )(owner_of, presence, whole, vmem(head))
    terms = [direct(head, 1)]
    *sums, own_sum = pl.pallas_call(
        sum_tail,
        in_specs=[SMEM] * 2 + [VMEM] * 2,
        out_specs=[VMEM] * (chips - 1),
        out_shape=[tile()] * (chips - 2) + [tile(dtype=f32)],
        name="sum_tail",
    )(owner_of, presence, whole, vmem(tail))
    for s, x in enumerate(sums, 2):
        terms.append(direct(x, s))

    def update(flag, outer, velocity, *refs):
        ins, (ship, next_outer, next_velocity) = refs[:chips], refs[chips:]
        count = sum(flag[r] for r in range(groups)).astype(f32)
        average = sum(x[...].astype(f32) for x in ins) / count
        moved = 0.9 * velocity[...] + average
        stepped = outer[...] - 0.7 * (average + 0.9 * moved)
        next_velocity[...] = moved
        next_outer[...] = stepped
        ship[...] = stepped.astype(bf16)

    shipped, new_outer, new_momentum = pl.pallas_call(
        update,
        in_specs=[SMEM] + [VMEM] * (2 + chips),
        out_specs=[VMEM] * 3,
        out_shape=[tile(), tile(dtype=f32), tile(dtype=f32)],
        name="update",
    )(presence, *map(vmem, [outer_params, momentum, own_sum, *terms]))

    got = [shipped]
    for s in range(1, chips):
        got.append(direct(shipped, s))
    other = [swap(shipped)]
    for s in range(1, chips):
        other.append(swap(got[s]))

    def store(plan, into, extra=()):
        arrays = [x for x, *_ in plan]
        kept_in = [] if into is None else [into]

        def body(owner, *refs):
            ins = refs[: len(arrays)]
            wholes = refs[len(arrays) : len(arrays) + len(extra)]
            out, *outs = refs[len(arrays) + len(extra) + len(kept_in) : -1]
            sem = refs[-1]
            chip, core = where()
            pieces = list(zip(wholes, outs))
            for x, (_, side, s) in zip(ins, plan):
                at = device(chip, 1 - core if side else core, s)
                pieces.append((x, out.at[:, columns(owner, at)]))
            copies = [pltpu.make_async_copy(a, b, sem.at[i]) for i, (a, b) in enumerate(pieces)]
            for copy in copies:
                copy.start()
            for copy in copies:
                copy.wait()

        return pl.pallas_call(
            body,
            in_specs=[SMEM] + [VMEM] * (len(arrays) + len(extra)) + [HBM] * len(kept_in),
            out_specs=[HBM] * (1 + len(extra)),
            out_shape=[pltpu.HBM((rows, groups * width), bf16)] + [pltpu.HBM((rows, width), f32)] * len(extra),
            scratch_shapes=[pltpu.SemaphoreType.DMA((len(arrays) + len(extra),))],
            input_output_aliases={1 + len(arrays): 0} if kept_in else {},
            name="store",
        )(owner_of, *map(vmem, [*arrays, *extra]), *kept_in)

    tail = chips - 1
    new_weights, new_outer, new_momentum = store([(shipped, False, 0)], None, (new_outer, new_momentum))
    for s in range(1, tail + 1):
        plan = [(got[s], False, s)] + [(other[k], True, k) for k in range(max(s - 2, 0), s - 1)]
        if s == tail:
            plan += [(other[k], True, k) for k in (tail - 1, tail)]
        (new_weights,) = store(plan, new_weights)
    return (new_weights, new_outer, new_momentum)


def solution(mesh):
    return jax.shard_map(
        shards,
        mesh=mesh,
        in_specs=(P("rep", "shard", None), P(), P(), P("shard", "rep"), P("shard", "rep")),
        out_specs=(P("shard", None), P("shard", "rep"), P("shard", "rep")),
        check_vma=False,
    )
```

```python
import jax
import jax.numpy as jnp
from jax import lax
from jax.experimental import pallas as pl
from jax.experimental.pallas import tpu as pltpu
from jax.sharding import PartitionSpec as P


SMEM = pl.BlockSpec(memory_space=pltpu.SMEM)
VMEM = pl.BlockSpec(memory_space=pltpu.VMEM)
ANY = pl.BlockSpec(memory_space=pl.ANY)
HBM = pl.BlockSpec(memory_space=pltpu.HBM)


def vmem(x):
    return pltpu.with_memory_space_constraint(x, pltpu.VMEM)


def smem(x):
    return pltpu.with_memory_space_constraint(x, pltpu.SMEM)


def shards(deltas, presence, owner_of, outer_params, momentum):
    groups = lax.axis_size("rep")
    chips = groups // 2
    rows = deltas.shape[1]
    width = deltas.shape[2] // groups
    bf16, f32 = jnp.bfloat16, jnp.float32
    flips = sorted(range(chips), key=lambda m: (m.bit_count(), m))

    def direct(x, s):
        return lax.ppermute(x, "rep", [(i, i ^ 2 * flips[s]) for i in range(groups)])

    def swap(x):
        return lax.ppermute(x, "rep", [(i, i ^ 1) for i in range(groups)])

    def where():
        me = lax.axis_index("rep")
        return me // 2, me % 2

    def device(chip, core, s):
        return (chip ^ flips[s]) * 2 + core

    def columns(owner, at):
        return pl.ds(pl.multiple_of(owner[at] * width, width), width)

    def own_flag(flag):
        return flag[lax.axis_index("rep")].astype(f32)

    def tile(*lead, dtype=bf16):
        return pltpu.VMEM((*lead, rows, width), dtype)

    later = [*range(2, chips), 0]

    def load(owner_hbm, flag_hbm, delta, owner, flag, whole, head, tail, sem):
        copies = [
            pltpu.make_async_copy(delta.at[0], whole, sem.at[0]),
            pltpu.make_async_copy(owner_hbm, owner, sem.at[1]),
            pltpu.make_async_copy(flag_hbm, flag, sem.at[2]),
        ]
        for copy in copies:
            copy.start()
        for copy in reversed(copies):
            copy.wait()
        chip, core = where()
        own = own_flag(flag)

        def masked(s):
            return (whole[:, columns(owner, device(chip, 1 - core, s))].astype(f32) * own).astype(bf16)

        head[...] = masked(1)
        for i, s in enumerate(later):
            tail[i] = masked(s)

    owner_of, presence, whole, head, tail = pl.pallas_call(
        load,
        in_specs=[ANY] * 3,
        out_specs=[SMEM] * 2 + [VMEM] * 3,
        out_shape=[pltpu.SMEM((groups,), jnp.int32)] * 2
        + [pltpu.VMEM((rows, groups * width), bf16), tile(), tile(chips - 1)],
        scratch_shapes=[pltpu.SemaphoreType.DMA((3,))],
        name="load",
    )(owner_of, presence, deltas)
    owner_of, presence, whole = smem(owner_of), smem(presence), vmem(whole)
    head = swap(head)
    tail = swap(tail)

    def add(owner, flag, whole, got, s):
        chip, core = where()
        mine = whole[:, columns(owner, device(chip, core, s))].astype(f32)
        return mine * own_flag(flag) + got.astype(f32)

    def sum_head(owner, flag, whole, got, out):
        out[...] = add(owner, flag, whole, got[...], 1).astype(bf16)

    def sum_tail(owner, flag, whole, got, *outs):
        for i, s in enumerate(later):
            outs[i][...] = add(owner, flag, whole, got[i], s).astype(outs[i].dtype)

    head = pl.pallas_call(
        sum_head,
        in_specs=[SMEM] * 2 + [VMEM] * 2,
        out_specs=VMEM,
        out_shape=tile(),
        name="sum_head",
    )(owner_of, presence, whole, vmem(head))
    terms = [direct(head, 1)]
    *sums, own_sum = pl.pallas_call(
        sum_tail,
        in_specs=[SMEM] * 2 + [VMEM] * 2,
        out_specs=[VMEM] * (chips - 1),
        out_shape=[tile()] * (chips - 2) + [tile(dtype=f32)],
        name="sum_tail",
    )(owner_of, presence, whole, vmem(tail))
    for s, x in enumerate(sums, 2):
        terms.append(direct(x, s))

    def update(flag, outer, velocity, *refs):
        ins, (ship, next_outer, next_velocity) = refs[:chips], refs[chips:]
        count = sum(flag[r] for r in range(groups)).astype(f32)
        average = sum(x[...].astype(f32) for x in ins) / count
        moved = 0.9 * velocity[...] + average
        stepped = outer[...] - 0.7 * (average + 0.9 * moved)
        next_velocity[...] = moved
        next_outer[...] = stepped
        ship[...] = stepped.astype(bf16)

    shipped, new_outer, new_momentum = pl.pallas_call(
        update,
        in_specs=[SMEM] + [VMEM] * (2 + chips),
        out_specs=[VMEM] * 3,
        out_shape=[tile(), tile(dtype=f32), tile(dtype=f32)],
        name="update",
    )(presence, *map(vmem, [outer_params, momentum, own_sum, *terms]))

    got = [shipped]
    for s in range(1, chips):
        got.append(direct(shipped, s))
    other = [swap(shipped)]
    for s in range(1, chips):
        other.append(swap(got[s]))

    def store(plan, into, extra=()):
        arrays = [x for x, *_ in plan]
        kept_in = [] if into is None else [into]

        def body(owner, *refs):
            ins = refs[: len(arrays)]
            wholes = refs[len(arrays) : len(arrays) + len(extra)]
            out, *outs = refs[len(arrays) + len(extra) + len(kept_in) : -1]
            sem = refs[-1]
            chip, core = where()
            pieces = list(zip(wholes, outs))
            for x, (_, side, s) in zip(ins, plan):
                at = device(chip, 1 - core if side else core, s)
                pieces.append((x, out.at[:, columns(owner, at)]))
            copies = [pltpu.make_async_copy(a, b, sem.at[i]) for i, (a, b) in enumerate(pieces)]
            for copy in copies:
                copy.start()
            for copy in copies:
                copy.wait()

        return pl.pallas_call(
            body,
            in_specs=[SMEM] + [VMEM] * (len(arrays) + len(extra)) + [HBM] * len(kept_in),
            out_specs=[HBM] * (1 + len(extra)),
            out_shape=[pltpu.HBM((rows, groups * width), bf16)] + [pltpu.HBM((rows, width), f32)] * len(extra),
            scratch_shapes=[pltpu.SemaphoreType.DMA((len(arrays) + len(extra),))],
            input_output_aliases={1 + len(arrays): 0} if kept_in else {},
            name="store",
        )(owner_of, *map(vmem, [*arrays, *extra]), *kept_in)

    tail = chips - 1
    new_weights, new_outer, new_momentum = store([(shipped, False, 0)], None, (new_outer, new_momentum))
    for s in range(1, tail):
        plan = [(got[s], False, s), *((other[k], True, k) for k in range(s - 1, s))]
        if s == tail - 1:
            plan += [(got[tail], False, tail), *((other[k], True, k) for k in range(tail - 1, tail))]
        (new_weights,) = store(plan, new_weights)
    (new_weights,) = store([(other[tail], True, tail)], new_weights)
    return (new_weights, new_outer, new_momentum)


def solution(mesh):
    return jax.shard_map(
        shards,
        mesh=mesh,
        in_specs=(P("rep", "shard", None), P(), P(), P("shard", "rep"), P("shard", "rep")),
        out_specs=(P("shard", None), P("shard", "rep"), P("shard", "rep")),
        check_vma=False,
    )
```

```python
import jax
import jax.numpy as jnp
from jax import lax
from jax.experimental import pallas as pl
from jax.experimental.pallas import tpu as pltpu
from jax.sharding import PartitionSpec as P


SMEM = pl.BlockSpec(memory_space=pltpu.SMEM)
VMEM = pl.BlockSpec(memory_space=pltpu.VMEM)
ANY = pl.BlockSpec(memory_space=pl.ANY)
HBM = pl.BlockSpec(memory_space=pltpu.HBM)


def vmem(x):
    return pltpu.with_memory_space_constraint(x, pltpu.VMEM)


def smem(x):
    return pltpu.with_memory_space_constraint(x, pltpu.SMEM)


def shards(deltas, presence, owner_of, outer_params, momentum):
    groups = lax.axis_size("rep")
    chips = groups // 2
    rows = deltas.shape[1]
    width = deltas.shape[2] // groups
    bf16, f32 = jnp.bfloat16, jnp.float32
    flips = sorted(range(chips), key=lambda m: (m.bit_count(), m))
    back = sorted(range(chips), key=lambda m: (m.bit_count(), -m))

    def direct(x, s, order):
        return lax.ppermute(x, "rep", [(i, i ^ 2 * order[s]) for i in range(groups)])

    def swap(x):
        return lax.ppermute(x, "rep", [(i, i ^ 1) for i in range(groups)])

    def where():
        me = lax.axis_index("rep")
        return me // 2, me % 2

    def device(chip, core, s):
        return (chip ^ flips[s]) * 2 + core

    def columns(owner, at):
        return pl.ds(pl.multiple_of(owner[at] * width, width), width)

    def own_flag(flag):
        return flag[lax.axis_index("rep")].astype(f32)

    def tile(*lead, dtype=bf16):
        return pltpu.VMEM((*lead, rows, width), dtype)

    later = [*range(2, chips), 0]

    def load(owner_hbm, flag_hbm, delta, owner, flag, whole, head, tail, sem):
        copies = [
            pltpu.make_async_copy(delta.at[0], whole, sem.at[0]),
            pltpu.make_async_copy(owner_hbm, owner, sem.at[1]),
            pltpu.make_async_copy(flag_hbm, flag, sem.at[2]),
        ]
        for copy in copies:
            copy.start()
        for copy in reversed(copies):
            copy.wait()
        chip, core = where()
        own = own_flag(flag)

        def masked(s):
            return (whole[:, columns(owner, device(chip, 1 - core, s))].astype(f32) * own).astype(bf16)

        head[...] = masked(1)
        for i, s in enumerate(later):
            tail[i] = masked(s)

    owner_of, presence, whole, head, tail = pl.pallas_call(
        load,
        in_specs=[ANY] * 3,
        out_specs=[SMEM] * 2 + [VMEM] * 3,
        out_shape=[pltpu.SMEM((groups,), jnp.int32)] * 2
        + [pltpu.VMEM((rows, groups * width), bf16), tile(), tile(chips - 1)],
        scratch_shapes=[pltpu.SemaphoreType.DMA((3,))],
        name="load",
    )(owner_of, presence, deltas)
    owner_of, presence, whole = smem(owner_of), smem(presence), vmem(whole)
    head = swap(head)
    tail = swap(tail)

    def add(owner, flag, whole, got, s):
        chip, core = where()
        mine = whole[:, columns(owner, device(chip, core, s))].astype(f32)
        return mine * own_flag(flag) + got.astype(f32)

    def sum_head(owner, flag, whole, got, out):
        out[...] = add(owner, flag, whole, got[...], 1).astype(bf16)

    def sum_tail(owner, flag, whole, got, *outs):
        for i, s in enumerate(later):
            outs[i][...] = add(owner, flag, whole, got[i], s).astype(outs[i].dtype)

    head = pl.pallas_call(
        sum_head,
        in_specs=[SMEM] * 2 + [VMEM] * 2,
        out_specs=VMEM,
        out_shape=tile(),
        name="sum_head",
    )(owner_of, presence, whole, vmem(head))
    terms = [direct(head, 1, flips)]
    *sums, own_sum = pl.pallas_call(
        sum_tail,
        in_specs=[SMEM] * 2 + [VMEM] * 2,
        out_specs=[VMEM] * (chips - 1),
        out_shape=[tile()] * (chips - 2) + [tile(dtype=f32)],
        name="sum_tail",
    )(owner_of, presence, whole, vmem(tail))
    for s, x in enumerate(sums, 2):
        terms.append(direct(x, s, flips))

    def update(flag, outer, velocity, *refs):
        ins, (ship, next_outer, next_velocity) = refs[:chips], refs[chips:]
        count = sum(flag[r] for r in range(groups)).astype(f32)
        average = sum(x[...].astype(f32) for x in ins) / count
        moved = 0.9 * velocity[...] + average
        stepped = outer[...] - 0.7 * (average + 0.9 * moved)
        next_velocity[...] = moved
        next_outer[...] = stepped
        ship[...] = stepped.astype(bf16)

    shipped, new_outer, new_momentum = pl.pallas_call(
        update,
        in_specs=[SMEM] + [VMEM] * (2 + chips),
        out_specs=[VMEM] * 3,
        out_shape=[tile(), tile(dtype=f32), tile(dtype=f32)],
        name="update",
    )(presence, *map(vmem, [outer_params, momentum, own_sum, *terms]))

    got = [shipped]
    for s in range(1, chips):
        got.append(direct(shipped, s, back))
    other = [swap(shipped)]
    for s in range(1, chips):
        other.append(swap(got[s]))

    def store(plan, into, extra=()):
        arrays = [x for x, *_ in plan]
        kept_in = [] if into is None else [into]

        def body(owner, *refs):
            ins = refs[: len(arrays)]
            wholes = refs[len(arrays) : len(arrays) + len(extra)]
            out, *outs = refs[len(arrays) + len(extra) + len(kept_in) : -1]
            sem = refs[-1]
            chip, core = where()
            pieces = list(zip(wholes, outs))
            for x, (_, side, s) in zip(ins, plan):
                at = (chip ^ back[s]) * 2 + (1 - core if side else core)
                pieces.append((x, out.at[:, columns(owner, at)]))
            copies = [pltpu.make_async_copy(a, b, sem.at[i]) for i, (a, b) in enumerate(pieces)]
            for copy in copies:
                copy.start()
            for copy in copies:
                copy.wait()

        return pl.pallas_call(
            body,
            in_specs=[SMEM] + [VMEM] * (len(arrays) + len(extra)) + [HBM] * len(kept_in),
            out_specs=[HBM] * (1 + len(extra)),
            out_shape=[pltpu.HBM((rows, groups * width), bf16)] + [pltpu.HBM((rows, width), f32)] * len(extra),
            scratch_shapes=[pltpu.SemaphoreType.DMA((len(arrays) + len(extra),))],
            input_output_aliases={1 + len(arrays): 0} if kept_in else {},
            name="store",
        )(owner_of, *map(vmem, [*arrays, *extra]), *kept_in)

    tail = chips - 1
    new_weights, new_outer, new_momentum = store([(shipped, False, 0)], None, (new_outer, new_momentum))
    for s in range(1, tail):
        plan = [(got[s], False, s), *((other[k], True, k) for k in range(s - 1, s))]
        if s == tail - 1:
            plan += [(got[tail], False, tail)]
        (new_weights,) = store(plan, new_weights)
    (new_weights,) = store([(other[k], True, k) for k in (tail - 1, tail)], new_weights)
    return (new_weights, new_outer, new_momentum)


def solution(mesh):
    return jax.shard_map(
        shards,
        mesh=mesh,
        in_specs=(P("rep", "shard", None), P(), P(), P("shard", "rep"), P("shard", "rep")),
        out_specs=(P("shard", None), P("shard", "rep"), P("shard", "rep")),
        check_vma=False,
    )
```
